32 devices in a mesh: job: 4 (over y, x), zero: 2 (over core), cols: 4 (over z).
Axes of the slice: x: 2, y: 2, z: 4, core: 2. Of those that a mesh axis runs over, the one named last changes fastest.
Arguments:
- weight_gate: bfloat16 [8192, 8192], P(('job', 'zero'), 'cols'), parts along dimension 0, may hold values from -0.1875 to 0.1875
- low_gate: bfloat16 [8192, 32], P(('job', 'zero')), parts along dimension 0, may hold values from -0.125 to 0.125
- high_gate: bfloat16 [128, 8192], P('job', 'cols'), parts along dimension 0, may hold values from -1 to 1
- weight_up: bfloat16 [8192, 8192], P(('job', 'zero'), 'cols'), parts along dimension 0, may hold values from -0.1875 to 0.1875
- low_up: bfloat16 [8192, 32], P(('job', 'zero')), parts along dimension 0, may hold values from -0.125 to 0.125
- high_up: bfloat16 [128, 8192], P('job', 'cols'), parts along dimension 0, may hold values from -1 to 1
- norm_train: float32 [8192], P(('job', 'zero', 'cols')), parts along dimension 0, may hold values from 0.25 to 1.75
- norm_step: float32 [8192], P(('job', 'zero', 'cols')), parts along dimension 0, may hold values from -0.3 to 0.3
Outputs:
- serving_gate: bfloat16 [8192, 8192], P('job', 'cols'), parts along dimension 0
- serving_up: bfloat16 [8192, 8192], P('job', 'cols'), parts along dimension 0
- column_gate: float32 [32768], P(('job', 'cols')), parts along dimension 0
- column_up: float32 [32768], P(('job', 'cols')), parts along dimension 0
- serve_norm: bfloat16 [8192], P('job'), parts along dimension 0
The draws below stay inside these ranges and needn't reach their ends.
There are 4 independent parts, one for each index of `job`. The reference program is written for one: setup_inputs(seed, part) draws one part's arguments, and reference() takes and returns one part's arrays. A program takes and returns all parts, laid end to end along the dimension named above; each array names one. Nothing has to cross between parts.
All inputs are finite; a program needn't handle non-finite values. Where the reference program divides by a largest or mean magnitude, that divisor is 1e-20 or more.
Results may differ from the reference program's by a relative error of at most 0.001.
Values may be sent and summed in bfloat16 or wider, within the bound.
A program may use at most 128 MiB of HBM per device.

```python
import jax
import jax.numpy as jnp

D_MODEL = 2048
D_INNER = 8192
RANK = 32


def raised(array, own_key, source, target, blocks, factor):
    def block_of(position):
        return (jnp.arange(array.shape[position]) // (array.shape[position] // blocks)).reshape((-1,) + (1,) * (array.ndim - 1 - position))

    one_side = jax.random.permutation(own_key, blocks)[block_of(target)]
    second = (block_of(target) + blocks // 2) % blocks
    return jnp.where((block_of(source) == one_side) | (block_of(source) == second), factor * array, array)


def level_of(key, dims, pieces, smallest, largest):
    def one(position, shards_of):
        draws = jax.random.uniform(jax.random.fold_in(jax.random.fold_in(key, 6), position), (shards_of,), jnp.float32, smallest / len(pieces), largest / len(pieces))
        return jnp.repeat(jnp.exp(draws), dims[position] // shards_of).reshape((-1,) + (1,) * (len(dims) - position - 1))

    level = one(*pieces[0])
    for cut in pieces[1:]:
        level = level * one(*cut)
    return level


def normal_values(rng, dims, scale, bound, pieces=(), dtype=jnp.bfloat16):
    entries = scale * jax.random.normal(rng, dims, jnp.float32)
    if pieces:
        entries = entries * level_of(rng, dims, pieces, -0.22, 0.18)
    return jnp.clip(entries, -bound, bound).astype(dtype)


def gaussian_with(own_key, dims, deviation, most, split, heavy, held_as=jnp.bfloat16):
    array = deviation * jax.random.normal(own_key, dims, jnp.float32)
    if split:
        array = array * level_of(own_key, dims, split, -0.22, 0.18)
    return jnp.clip(raised(array, jax.random.fold_in(own_key, 3), *heavy), -most, most).astype(held_as)


def setup_inputs(seed: int = 0, part: int = 0) -> dict:
    keys = jax.random.split(jax.random.key(seed), 9)
    part_keys = jax.random.split(jax.random.fold_in(keys[8], part), 9)
    weight_gate = gaussian_with(part_keys[0], (D_MODEL, D_INNER), D_MODEL ** -0.5, 0.1875, ((0, 2), (1, 4)), (0, 1, 4, 2.0))
    low_gate = normal_values(part_keys[1], (D_MODEL, RANK), D_MODEL ** -0.5, 0.125, ((0, 2),))
    high_gate = normal_values(part_keys[2], (RANK, D_INNER), RANK ** -0.5, 1.0, ((1, 4),))
    weight_up = gaussian_with(part_keys[3], (D_MODEL, D_INNER), D_MODEL ** -0.5, 0.1875, ((0, 2), (1, 4)), (0, 1, 4, 2.0))
    low_up = normal_values(part_keys[4], (D_MODEL, RANK), D_MODEL ** -0.5, 0.125, ((0, 2),))
    high_up = normal_values(part_keys[5], (RANK, D_INNER), RANK ** -0.5, 1.0, ((1, 4),))
    norm_train = jnp.clip(1.0 + 0.15 * jax.random.normal(part_keys[6], (D_MODEL,), jnp.float32), 0.25, 1.75)
    norm_step = jnp.clip(jax.random.uniform(part_keys[7], (D_MODEL,), jnp.float32, -0.3, 0.3) * level_of(part_keys[7], (D_MODEL,), ((0, 8),), -0.4, 0.0), -0.3, 0.3)
    return {"weight_gate": weight_gate, "low_gate": low_gate, "high_gate": high_gate, "weight_up": weight_up, "low_up": low_up, "high_up": high_up, "norm_train": norm_train, "norm_step": norm_step}


mix_rate = 2.0


def reference(weight_gate, low_gate, high_gate, weight_up, low_up, high_up, norm_train, norm_step):
    whole_gate = weight_gate.astype(jnp.float32) + mix_rate * jnp.dot(low_gate, high_gate, preferred_element_type=jnp.float32)
    whole_up = weight_up.astype(jnp.float32) + mix_rate * jnp.dot(low_up, high_up, preferred_element_type=jnp.float32)
    column_gate = jnp.max(jnp.abs(whole_gate), axis=0)
    serving_gate = (whole_gate / column_gate).astype(jnp.bfloat16)
    column_up = jnp.max(jnp.abs(whole_up), axis=0)
    serving_up = (whole_up / column_up).astype(jnp.bfloat16)
    serve_norm = (norm_train + norm_step).astype(jnp.bfloat16)
    return serving_gate, serving_up, column_gate, column_up, serve_norm
```

```python
import functools

import jax
import jax.numpy as jnp
from jax import lax
from jax.experimental import pallas as pl
from jax.experimental.pallas import tpu as pltpu
from jax.sharding import PartitionSpec as P

mix_rate = 2.0
MESH = pl.DeviceIdType.MESH


def small_kernel(zeros, cols, lows, *refs):
    train_ref, step_ref = refs[:2]
    low_refs = refs[2:2 + lows]
    norm_ref = refs[2 + lows]
    got_refs = refs[3 + lows:3 + 2 * lows]
    landed = refs[3 + 2 * lows:3 + 3 * lows]
    mine, slots, norm_send, norm_recv, low_send, low_recv = refs[3 + 3 * lows:]
    group = zeros * cols
    zero, col = lax.axis_index("zero"), lax.axis_index("cols")
    me = zero * cols + col

    def device(rank):
        return {"zero": rank // cols, "cols": lax.rem(rank, cols)}

    barrier = pltpu.get_barrier_semaphore()
    for s in range(1, group):
        pl.semaphore_signal(barrier, inc=1, device_id=device(lax.rem(me + s, group)), device_id_type=MESH)
    mine[...] = train_ref[...] + step_ref[...]
    pl.semaphore_wait(barrier, group - 1)

    copies = []
    for s in range(1, zeros):
        for k in range(lows):
            copies.append(pltpu.make_async_remote_copy(
                src_ref=low_refs[k], dst_ref=landed[k].at[s - 1],
                send_sem=low_send.at[k, s - 1], recv_sem=low_recv.at[k, s - 1],
                device_id={"zero": lax.rem(zero + s, zeros), "cols": col}, device_id_type=MESH))
            copies[-1].start()
    for s in range(1, group):
        copy = pltpu.make_async_remote_copy(
            src_ref=mine, dst_ref=slots.at[me],
            send_sem=norm_send.at[s - 1], recv_sem=norm_recv.at[s - 1],
            device_id=device(lax.rem(me + s, group)), device_id_type=MESH)
        copy.start()
        copies.append(copy)
    for k in range(lows):
        got_refs[k][0] = low_refs[k][...].T
    for copy in copies:
        copy.wait()
    for k in range(lows):
        for s in range(1, zeros):
            got_refs[k][s] = landed[k][s - 1].T
    norm_ref[...] = slots[...].astype(norm_ref.dtype)
    norm_ref[me] = mine[...].astype(norm_ref.dtype)


def exchange_small(zeros, cols, train, step, lows):
    group = zeros * cols
    piece = train.shape[0]
    outs = pl.pallas_call(
        functools.partial(small_kernel, zeros, cols, len(lows)),
        out_shape=[jax.ShapeDtypeStruct((group, 1, piece), jnp.bfloat16)]
        + [jax.ShapeDtypeStruct((zeros,) + low.shape, low.dtype) for low in lows],
        in_specs=[pl.BlockSpec(memory_space=pltpu.VMEM)] * (2 + len(lows)),
        out_specs=[pl.BlockSpec(memory_space=pltpu.VMEM)] * (1 + len(lows)),
        scratch_shapes=[
            pltpu.VMEM((zeros - 1,) + low.shape[::-1], low.dtype) for low in lows
        ] + [
            pltpu.VMEM((1, piece), jnp.float32),
            pltpu.VMEM((group, 1, piece), jnp.float32),
            pltpu.SemaphoreType.DMA((group - 1,)),
            pltpu.SemaphoreType.DMA((group - 1,)),
            pltpu.SemaphoreType.DMA((len(lows), zeros - 1)),
            pltpu.SemaphoreType.DMA((len(lows), zeros - 1)),
        ],
        cost_estimate=pl.CostEstimate(flops=0, bytes_accessed=2 ** 22, transcendentals=0),
        compiler_params=pltpu.CompilerParams(collective_id=0, has_side_effects=True),
    )(train.reshape(1, piece), step.reshape(1, piece), *[low.T for low in lows])
    return outs[0].reshape(group * piece), outs[1:]


def merge_kernel(zeros, chunk, *refs):
    weight_refs = refs[:zeros]
    low_ref, high_ref, out_ref, column_ref, whole = refs[zeros:]
    zero = lax.axis_index("zero")
    rows, width = weight_refs[0].shape
    high = high_ref[...] * jnp.bfloat16(mix_rate)
    most = jnp.zeros((8, width), jnp.float32)
    for s in range(zeros):
        def step(i, most, s=s):
            at = pl.ds(pl.multiple_of(i * chunk, chunk), chunk)
            low = low_ref[s, at, :]
            value = weight_refs[s][at, :].astype(jnp.float32) + jnp.dot(
                low, high, preferred_element_type=jnp.float32)
            whole[s, at, :] = value
            return jnp.maximum(most, jnp.max(jnp.abs(value).reshape(chunk // 8, 8, width), axis=0))
        most = lax.fori_loop(0, rows // chunk, step, most, unroll=True)
    column = jnp.max(most, axis=0, keepdims=True)
    column_ref[...] = column
    scale = 1.0 / column
    for s in range(zeros):
        base = lax.rem(zero - s + zeros, zeros) * rows

        def put(i, carry, s=s, base=base):
            start = pl.multiple_of(i * chunk, chunk)
            out_ref[pl.ds(pl.multiple_of(base + start, chunk), chunk), :] = (
                whole[s, pl.ds(start, chunk), :] * scale).astype(out_ref.dtype)
            return carry
        lax.fori_loop(0, rows // chunk, put, 0, unroll=True)


def merge(zeros, weights, low, high):
    rows, columns = weights[0].shape
    rank = low.shape[2]
    width = min(256, columns)
    chunk = min(128, rows)
    serving, column = pl.pallas_call(
        functools.partial(merge_kernel, zeros, chunk),
        grid=(columns // width,),
        out_shape=[
            jax.ShapeDtypeStruct((rows * zeros, columns), jnp.bfloat16),
            jax.ShapeDtypeStruct((1, columns), jnp.float32),
        ],
        in_specs=[pl.BlockSpec((rows, width), lambda j: (0, j))] * zeros + [
            pl.BlockSpec((zeros, rows, rank), lambda j: (0, 0, 0)),
            pl.BlockSpec((rank, width), lambda j: (0, j)),
        ],
        out_specs=[
            pl.BlockSpec((rows * zeros, width), lambda j: (0, j)),
            pl.BlockSpec((1, width), lambda j: (0, j)),
        ],
        scratch_shapes=[pltpu.VMEM((zeros, rows, width), jnp.float32)],
        cost_estimate=pl.CostEstimate(
            flops=2 * rows * zeros * columns * rank,
            bytes_accessed=4 * rows * zeros * columns, transcendentals=0),
        compiler_params=pltpu.CompilerParams(dimension_semantics=("arbitrary",)),
    )(*weights, low, high)
    return serving, column.reshape(columns)


def per_device(zeros, cols, weight_gate, low_gate, high_gate, weight_up, low_up, high_up, norm_train, norm_step):
    def moved(array):
        return [array] + [
            lax.ppermute(array, "zero", [(i, (i + s) % zeros) for i in range(zeros)])
            for s in range(1, zeros)
        ]

    gates, ups = moved(weight_gate), moved(weight_up)
    serve_norm, (all_gate, all_up) = exchange_small(
        zeros, cols, norm_train, norm_step, (low_gate, low_up))
    serving_gate, column_gate = merge(zeros, gates, all_gate, high_gate)
    serving_up, column_up = merge(zeros, ups, all_up, high_up)
    return (serving_gate, serving_up, column_gate, column_up, serve_norm)


def solution(mesh):
    in_specs = (
        P(("job", "zero"), "cols"),
        P(("job", "zero"), None),
        P("job", "cols"),
        P(("job", "zero"), "cols"),
        P(("job", "zero"), None),
        P("job", "cols"),
        P(("job", "zero", "cols")),
        P(("job", "zero", "cols")),
    )
    out_specs = (
        P("job", "cols"),
        P("job", "cols"),
        P(("job", "cols")),
        P(("job", "cols")),
        P("job"),
    )
    return jax.shard_map(
        functools.partial(per_device, mesh.shape["zero"], mesh.shape["cols"]),
        mesh=mesh, in_specs=in_specs, out_specs=out_specs, check_vma=False
    )
```

```python
import functools

import jax
import jax.numpy as jnp
from jax import lax
from jax.experimental import pallas as pl
from jax.experimental.pallas import tpu as pltpu
from jax.sharding import PartitionSpec as P

mix_rate = 2.0
MESH = pl.DeviceIdType.MESH


def first_kernel(zeros, cols, lows, weight_ref, *refs):
    train_ref, step_ref = refs[:2]
    low_refs = refs[2:2 + lows]
    norm_ref = refs[2 + lows]
    got_refs = refs[3 + lows:3 + 2 * lows]
    moved_refs = refs[3 + 2 * lows:2 + 2 * lows + zeros]
    refs = refs[2 + 2 * lows + zeros:]
    landed = refs[:lows]
    mine, slots, norm_send, norm_recv, low_send, low_recv, weight_send, weight_recv = refs[lows:]
    group = zeros * cols
    zero, col = lax.axis_index("zero"), lax.axis_index("cols")
    me = zero * cols + col

    def device(rank):
        return {"zero": rank // cols, "cols": lax.rem(rank, cols)}

    barrier = pltpu.get_barrier_semaphore()
    for s in range(1, group):
        pl.semaphore_signal(barrier, inc=1, device_id=device(lax.rem(me + s, group)), device_id_type=MESH)
    mine[...] = train_ref[...] + step_ref[...]
    pl.semaphore_wait(barrier, group - 1)

    copies = []
    for s in range(1, zeros):
        for k in range(lows):
            copies.append(pltpu.make_async_remote_copy(
                src_ref=low_refs[k], dst_ref=landed[k].at[s - 1],
                send_sem=low_send.at[k, s - 1], recv_sem=low_recv.at[k, s - 1],
                device_id={"zero": lax.rem(zero + s, zeros), "cols": col}, device_id_type=MESH))
            copies[-1].start()
    for s in range(1, zeros):
        copies.append(pltpu.make_async_remote_copy(
            src_ref=weight_ref, dst_ref=moved_refs[s - 1],
            send_sem=weight_send.at[s - 1], recv_sem=weight_recv.at[s - 1],
            device_id={"zero": lax.rem(zero + s, zeros), "cols": col}, device_id_type=MESH))
    for s in range(1, group):
        copy = pltpu.make_async_remote_copy(
            src_ref=mine, dst_ref=slots.at[me],
            send_sem=norm_send.at[s - 1], recv_sem=norm_recv.at[s - 1],
            device_id=device(lax.rem(me + s, group)), device_id_type=MESH)
        copy.start()
        copies.append(copy)
    for copy in copies[lows * (zeros - 1):(1 + lows) * (zeros - 1)]:
        copy.start()
    for k in range(lows):
        got_refs[k][0] = low_refs[k][...].T
    for copy in copies:
        copy.wait()
    for k in range(lows):
        for s in range(1, zeros):
            got_refs[k][s] = landed[k][s - 1].T
    slots[me] = mine[...]
    norm_ref[...] = jnp.concatenate([slots[g] for g in range(group)], axis=0).astype(norm_ref.dtype)


def exchange_first(zeros, cols, weight, train, step, lows):
    group = zeros * cols
    lanes = 128 if train.shape[0] % 128 == 0 else train.shape[0]
    tall = train.shape[0] // lanes
    outs = pl.pallas_call(
        functools.partial(first_kernel, zeros, cols, len(lows)),
        out_shape=[jax.ShapeDtypeStruct((group * tall, lanes), jnp.bfloat16)]
        + [jax.ShapeDtypeStruct((zeros,) + low.shape, low.dtype) for low in lows]
        + [jax.ShapeDtypeStruct(weight.shape, weight.dtype)] * (zeros - 1),
        in_specs=[pl.BlockSpec(memory_space=pl.ANY)] + [pl.BlockSpec(memory_space=pltpu.VMEM)] * (2 + len(lows)),
        out_specs=[pl.BlockSpec(memory_space=pltpu.VMEM)] * (1 + len(lows))
        + [pl.BlockSpec(memory_space=pl.ANY)] * (zeros - 1),
        scratch_shapes=[
            pltpu.VMEM((zeros - 1,) + low.shape[::-1], low.dtype) for low in lows
        ] + [
            pltpu.VMEM((tall, lanes), jnp.float32),
            pltpu.VMEM((group, tall, lanes), jnp.float32),
            pltpu.SemaphoreType.DMA((group - 1,)),
            pltpu.SemaphoreType.DMA((group - 1,)),
            pltpu.SemaphoreType.DMA((len(lows), zeros - 1)),
            pltpu.SemaphoreType.DMA((len(lows), zeros - 1)),
            pltpu.SemaphoreType.DMA((zeros - 1,)),
            pltpu.SemaphoreType.DMA((zeros - 1,)),
        ],
        cost_estimate=pl.CostEstimate(flops=0, bytes_accessed=2 ** 22, transcendentals=0),
        compiler_params=pltpu.CompilerParams(collective_id=0, has_side_effects=True),
    )(weight, train.reshape(tall, lanes), step.reshape(tall, lanes), *[low.T for low in lows])
    return outs[0].reshape(group * tall * lanes), outs[1:1 + len(lows)], outs[1 + len(lows):]


def merge_kernel(zeros, chunk, *refs):
    weight_refs = refs[:zeros]
    low_ref, high_ref, out_ref, column_ref, whole = refs[zeros:]
    zero = lax.axis_index("zero")
    rows, width = weight_refs[0].shape
    high = high_ref[...] * jnp.bfloat16(mix_rate)
    most = jnp.zeros((8, width), jnp.float32)
    for s in range(zeros):
        def step(i, most, s=s):
            at = pl.ds(pl.multiple_of(i * chunk, chunk), chunk)
            low = low_ref[s, at, :]
            value = weight_refs[s][at, :].astype(jnp.float32) + jnp.dot(
                low, high, preferred_element_type=jnp.float32)
            whole[s, at, :] = value
            return jnp.maximum(most, jnp.max(jnp.abs(value).reshape(chunk // 8, 8, width), axis=0))
        most = lax.fori_loop(0, rows // chunk, step, most, unroll=True)
    column = jnp.max(most, axis=0, keepdims=True)
    column_ref[...] = column
    scale = 1.0 / column
    for s in range(zeros):
        base = lax.rem(zero - s + zeros, zeros) * rows

        def put(i, carry, s=s, base=base):
            start = pl.multiple_of(i * chunk, chunk)
            out_ref[pl.ds(pl.multiple_of(base + start, chunk), chunk), :] = (
                whole[s, pl.ds(start, chunk), :] * scale).astype(out_ref.dtype)
            return carry
        lax.fori_loop(0, rows // chunk, put, 0, unroll=True)


def merge(zeros, weights, low, high):
    rows, columns = weights[0].shape
    rank = low.shape[2]
    width = min(512, columns)
    chunk = min(128, rows)
    serving, column = pl.pallas_call(
        functools.partial(merge_kernel, zeros, chunk),
        grid=(columns // width,),
        out_shape=[
            jax.ShapeDtypeStruct((rows * zeros, columns), jnp.bfloat16),
            jax.ShapeDtypeStruct((1, columns), jnp.float32),
        ],
        in_specs=[pl.BlockSpec((rows, width), lambda j: (0, j))] * zeros + [
            pl.BlockSpec((zeros, rows, rank), lambda j: (0, 0, 0)),
            pl.BlockSpec((rank, width), lambda j: (0, j)),
        ],
        out_specs=[
            pl.BlockSpec((rows * zeros, width), lambda j: (0, j)),
            pl.BlockSpec((1, width), lambda j: (0, j)),
        ],
        scratch_shapes=[pltpu.VMEM((zeros, rows, width), jnp.float32)],
        cost_estimate=pl.CostEstimate(
            flops=2 * rows * zeros * columns * rank,
            bytes_accessed=4 * rows * zeros * columns, transcendentals=0),
        compiler_params=pltpu.CompilerParams(dimension_semantics=("arbitrary",), vmem_limit_bytes=60 * 2 ** 20),
    )(*weights, low, high)
    return serving, column.reshape(columns)


def per_device(zeros, cols, weight_gate, low_gate, high_gate, weight_up, low_up, high_up, norm_train, norm_step):
    def moved(array):
        return [array] + [
            lax.ppermute(array, "zero", [(i, (i + s) % zeros) for i in range(zeros)])
            for s in range(1, zeros)
        ]

    serve_norm, (all_gate, all_up), gates = exchange_first(
        zeros, cols, weight_gate, norm_train, norm_step, (low_gate, low_up))
    weight_up, all_up = lax.optimization_barrier((weight_up, all_up))
    ups = moved(weight_up)
    serving_gate, column_gate = merge(zeros, [weight_gate, *gates], all_gate, high_gate)
    serving_up, column_up = merge(zeros, ups, all_up, high_up)
    return (serving_gate, serving_up, column_gate, column_up, serve_norm)


def solution(mesh):
    in_specs = (
        P(("job", "zero"), "cols"),
        P(("job", "zero"), None),
        P("job", "cols"),
        P(("job", "zero"), "cols"),
        P(("job", "zero"), None),
        P("job", "cols"),
        P(("job", "zero", "cols")),
        P(("job", "zero", "cols")),
    )
    out_specs = (
        P("job", "cols"),
        P("job", "cols"),
        P(("job", "cols")),
        P(("job", "cols")),
        P("job"),
    )
    return jax.shard_map(
        functools.partial(per_device, mesh.shape["zero"], mesh.shape["cols"]),
        mesh=mesh, in_specs=in_specs, out_specs=out_specs, check_vma=False
    )
```

```python
import functools

import jax
import jax.numpy as jnp
from jax import lax
from jax.experimental import pallas as pl
from jax.experimental.pallas import tpu as pltpu
from jax.sharding import PartitionSpec as P

mix_rate = 2.0
MESH = pl.DeviceIdType.MESH


def small_kernel(zeros, cols, lows, *refs):
    train_ref, step_ref = refs[:2]
    low_refs = refs[2:2 + lows]
    norm_ref = refs[2 + lows]
    got_refs = refs[3 + lows:3 + 2 * lows]
    landed = refs[3 + 2 * lows:3 + 3 * lows]
    mine, slots, norm_send, norm_recv, low_send, low_recv = refs[3 + 3 * lows:]
    group = zeros * cols
    zero, col = lax.axis_index("zero"), lax.axis_index("cols")
    me = zero * cols + col

    def device(rank):
        return {"zero": rank // cols, "cols": lax.rem(rank, cols)}

    barrier = pltpu.get_barrier_semaphore()
    for s in range(1, group):
        pl.semaphore_signal(barrier, inc=1, device_id=device(lax.rem(me + s, group)), device_id_type=MESH)
    mine[...] = train_ref[...] + step_ref[...]
    pl.semaphore_wait(barrier, group - 1)

    copies = []
    for s in range(1, zeros):
        for k in range(lows):
            copies.append(pltpu.make_async_remote_copy(
                src_ref=low_refs[k], dst_ref=landed[k].at[s - 1],
                send_sem=low_send.at[k, s - 1], recv_sem=low_recv.at[k, s - 1],
                device_id={"zero": lax.rem(zero + s, zeros), "cols": col}, device_id_type=MESH))
            copies[-1].start()
    for s in range(1, group):
        copy = pltpu.make_async_remote_copy(
            src_ref=mine, dst_ref=slots.at[me],
            send_sem=norm_send.at[s - 1], recv_sem=norm_recv.at[s - 1],
            device_id=device(lax.rem(me + s, group)), device_id_type=MESH)
        copy.start()
        copies.append(copy)
    for k in range(lows):
        got_refs[k][0] = low_refs[k][...].T
    for copy in copies:
        copy.wait()
    for k in range(lows):
        for s in range(1, zeros):
            got_refs[k][s] = landed[k][s - 1].T
    slots[me] = mine[...]
    norm_ref[...] = jnp.concatenate([slots[g] for g in range(group)], axis=0).astype(norm_ref.dtype)


def exchange_small(zeros, cols, train, step, lows):
    group = zeros * cols
    lanes = 128 if train.shape[0] % 128 == 0 else train.shape[0]
    tall = train.shape[0] // lanes
    outs = pl.pallas_call(
        functools.partial(small_kernel, zeros, cols, len(lows)),
        out_shape=[jax.ShapeDtypeStruct((group * tall, lanes), jnp.bfloat16)]
        + [jax.ShapeDtypeStruct((zeros,) + low.shape, low.dtype) for low in lows],
        in_specs=[pl.BlockSpec(memory_space=pltpu.VMEM)] * (2 + len(lows)),
        out_specs=[pl.BlockSpec(memory_space=pltpu.VMEM)] * (1 + len(lows)),
        scratch_shapes=[
            pltpu.VMEM((zeros - 1,) + low.shape[::-1], low.dtype) for low in lows
        ] + [
            pltpu.VMEM((tall, lanes), jnp.float32),
            pltpu.VMEM((group, tall, lanes), jnp.float32),
            pltpu.SemaphoreType.DMA((group - 1,)),
            pltpu.SemaphoreType.DMA((group - 1,)),
            pltpu.SemaphoreType.DMA((len(lows), zeros - 1)),
            pltpu.SemaphoreType.DMA((len(lows), zeros - 1)),
        ],
        cost_estimate=pl.CostEstimate(flops=0, bytes_accessed=2 ** 22, transcendentals=0),
        compiler_params=pltpu.CompilerParams(collective_id=0, has_side_effects=True),
    )(train.reshape(tall, lanes), step.reshape(tall, lanes), *[low.T for low in lows])
    return outs[0].reshape(group * tall * lanes), outs[1:]


def merge_kernel(zeros, chunk, *refs):
    weight_refs = refs[:zeros]
    low_ref, high_ref, out_ref, column_ref, whole = refs[zeros:]
    zero = lax.axis_index("zero")
    rows, width = weight_refs[0].shape
    high = high_ref[...] * jnp.bfloat16(mix_rate)
    most = jnp.zeros((8, width), jnp.float32)
    for s in range(zeros):
        def step(i, most, s=s):
            at = pl.ds(pl.multiple_of(i * chunk, chunk), chunk)
            low = low_ref[s, at, :]
            value = weight_refs[s][at, :].astype(jnp.float32) + jnp.dot(
                low, high, preferred_element_type=jnp.float32)
            whole[s, at, :] = value
            return jnp.maximum(most, jnp.max(jnp.abs(value).reshape(chunk // 8, 8, width), axis=0))
        most = lax.fori_loop(0, rows // chunk, step, most, unroll=True)
    column = jnp.max(most, axis=0, keepdims=True)
    column_ref[...] = column
    scale = 1.0 / column
    for s in range(zeros):
        base = lax.rem(zero - s + zeros, zeros) * rows

        def put(i, carry, s=s, base=base):
            start = pl.multiple_of(i * chunk, chunk)
            out_ref[pl.ds(pl.multiple_of(base + start, chunk), chunk), :] = (
                whole[s, pl.ds(start, chunk), :] * scale).astype(out_ref.dtype)
            return carry
        lax.fori_loop(0, rows // chunk, put, 0, unroll=True)


def merge(zeros, weights, low, high):
    rows, columns = weights[0].shape
    rank = low.shape[2]
    width = min(512, columns)
    chunk = min(128, rows)
    serving, column = pl.pallas_call(
        functools.partial(merge_kernel, zeros, chunk),
        grid=(columns // width,),
        out_shape=[
            jax.ShapeDtypeStruct((rows * zeros, columns), jnp.bfloat16),
            jax.ShapeDtypeStruct((1, columns), jnp.float32),
        ],
        in_specs=[pl.BlockSpec((rows, width), lambda j: (0, j))] * zeros + [
            pl.BlockSpec((zeros, rows, rank), lambda j: (0, 0, 0)),
            pl.BlockSpec((rank, width), lambda j: (0, j)),
        ],
        out_specs=[
            pl.BlockSpec((rows * zeros, width), lambda j: (0, j)),
            pl.BlockSpec((1, width), lambda j: (0, j)),
        ],
        scratch_shapes=[pltpu.VMEM((zeros, rows, width), jnp.float32)],
        cost_estimate=pl.CostEstimate(
            flops=2 * rows * zeros * columns * rank,
            bytes_accessed=4 * rows * zeros * columns, transcendentals=0),
        compiler_params=pltpu.CompilerParams(dimension_semantics=("arbitrary",), vmem_limit_bytes=60 * 2 ** 20),
    )(*weights, low, high)
    return serving, column.reshape(columns)


def per_device(zeros, cols, weight_gate, low_gate, high_gate, weight_up, low_up, high_up, norm_train, norm_step):
    def moved(array):
        return [array] + [
            lax.ppermute(array, "zero", [(i, (i + s) % zeros) for i in range(zeros)])
            for s in range(1, zeros)
        ]

    gates, ups = moved(weight_gate), moved(weight_up)
    serve_norm, (all_gate, all_up) = exchange_small(
        zeros, cols, norm_train, norm_step, (low_gate, low_up))
    serving_gate, column_gate = merge(zeros, gates, all_gate, high_gate)
    serving_up, column_up = merge(zeros, ups, all_up, high_up)
    return (serving_gate, serving_up, column_gate, column_up, serve_norm)


def solution(mesh):
    in_specs = (
        P(("job", "zero"), "cols"),
        P(("job", "zero"), None),
        P("job", "cols"),
        P(("job", "zero"), "cols"),
        P(("job", "zero"), None),
        P("job", "cols"),
        P(("job", "zero", "cols")),
        P(("job", "zero", "cols")),
    )
    out_specs = (
        P("job", "cols"),
        P("job", "cols"),
        P(("job", "cols")),
        P(("job", "cols")),
        P("job"),
    )
    return jax.shard_map(
        functools.partial(per_device, mesh.shape["zero"], mesh.shape["cols"]),
        mesh=mesh, in_specs=in_specs, out_specs=out_specs, check_vma=False
    )
```
